32 devices in a mesh: pop: 8 (over z, y), mp: 4 (over x, core).
Axes of the slice: x: 2, y: 2, z: 4, core: 2. Of those that a mesh axis runs over, the one named last changes fastest.
Arguments:
- token_ids: int32 [96, 4, 16], P('pop'), may hold values from 0 to 255
- fitness_ranks: int32 [96], P('pop'), may hold values from 0 to 143, as said below
- embedding: bfloat16 [256, 4096], P(None, 'mp'), may hold values from -6 to 6
- mix_weights: bfloat16 [2, 4096, 4096], P(None, 'mp'), may hold values from -0.09375 to 0.09375
- factors_in: bfloat16 [2, 96, 4, 4096], P(None, 'pop', None, 'mp'), may hold values from -6 to 6
- factors_out: bfloat16 [2, 96, 4, 4096], P(None, 'pop'), may hold values from -6 to 6
- decay_rates: float32 [2, 4096], P(None, 'mp'), may hold values from 0.2 to 0.98
- norm_gain: float32 [2, 4096], P(None, 'mp'), may hold values from 0.1 to 1.9
- reward_dir: float32 [4096], P('mp'), may hold values from -6 to 6
Outputs:
- final_features: bfloat16 [96, 4, 4096], P('pop', None, 'mp')
- scores: float32 [96, 4], P('pop')
- weight_step: float32 [2, 4096, 4096], P(None, 'mp', 'pop')
The draws below stay inside these ranges and needn't reach their ends.
Inputs may be any that keep to these rules, and one draw needn't show every extreme that they name: `fitness_ranks`: ranks may repeat.
All inputs are finite; a program needn't handle non-finite values.
Results may differ from the reference program's by a relative error of at most 0.023.
Values may be sent and summed in bfloat16 or wider, within the bound.
A program may use at most 128 MiB of HBM per device.

```python
import jax
import jax.numpy as jnp
from jax import lax

D = 4096
VOCAB = 256
RANK = 4
LAYERS = 2
STEPS = 16
SEQS = 4
MEMBERS = 96
N_MP = 4


def draw_fitness_ranks(key, part):
    member_idx = jnp.arange(MEMBERS, dtype=jnp.int32)
    upper = MEMBERS // 2 + member_idx + 1
    drawn = jax.random.randint(jax.random.fold_in(key, 11), (MEMBERS,), 0, upper, dtype=jnp.int32)
    drawn = drawn.at[MEMBERS - 1].set(MEMBERS + MEMBERS // 2 - 1)
    drawn = drawn.at[0].set(0)
    return drawn


def place_ends(array, rng, smallest, high):
    dims = array.shape
    index_at = [jax.random.randint(jax.random.fold_in(rng, axis), (), 0, dims[axis]) for axis in range(len(dims))]
    array = array.at[tuple(index_at)].set(smallest)
    longest = dims.index(max(dims))
    index_at[longest] = (index_at[longest] + 1) % dims[longest]
    return array.at[tuple(index_at)].set(high)


def block_levels(stream_key, dims, pieces, smallest, top_value):
    gain, own = 1.0, jax.random.fold_in(stream_key, 6)
    for axis_at, blocks in pieces:
        heights = jnp.exp(jax.random.uniform(jax.random.fold_in(own, axis_at), (blocks,), jnp.float32, smallest / len(pieces), top_value / len(pieces)))
        gain = gain * jnp.repeat(heights, dims[axis_at] // blocks).reshape([-1 if axis == axis_at else 1 for axis in range(len(dims))])
    return gain


def centred(own_key, extent, spread, reach, shards=(), kind=jnp.bfloat16):
    level = block_levels(own_key, extent, shards, -0.22, 0.18) if shards else 1.0
    entries = jax.random.normal(own_key, extent, jnp.float32) * spread * level
    return jnp.minimum(jnp.maximum(entries, -reach), reach).astype(kind)


def setup_inputs(seed: int = 0) -> dict:
    seeds = jax.random.split(jax.random.key(seed), 10)
    token_ids = place_ends(jax.random.randint(seeds[0], (MEMBERS, SEQS, STEPS), 0, VOCAB), jax.random.fold_in(seeds[0], 1), 0, VOCAB - 1).astype(jnp.int32)
    fitness_ranks = draw_fitness_ranks(jax.random.fold_in(seeds[9], 71), 0)
    embedding = centred(seeds[2], (VOCAB, D), 1.0, 6.0, ((1, 4),))
    mix_weights = centred(seeds[3], (LAYERS, D, D), D ** -0.5, 0.09375, ((1, 4),))
    factors_in = centred(seeds[4], (LAYERS, MEMBERS, RANK, D), 1.0, 6.0, ((1, 8), (3, 4)))
    factors_out = centred(seeds[5], (LAYERS, MEMBERS, RANK, D), 1.0, 6.0, ((1, 8),))
    decay_rates = jnp.clip(0.2 + 0.78000002 * jax.random.uniform(seeds[6], (LAYERS, D), jnp.float32) ** block_levels(seeds[6], (LAYERS, D), ((1, 4),), -0.2, 0.2), 0.2, 0.98)
    norm_gain = jnp.clip(1.0 + 0.18 * jax.random.normal(seeds[7], (LAYERS, D), jnp.float32), 0.1, 1.9)
    reward_dir = centred(seeds[8], (D,), 1.0, 6.0, ((0, 4),), jnp.float32)
    return dict(token_ids=token_ids, fitness_ranks=fitness_ranks, embedding=embedding, mix_weights=mix_weights, factors_in=factors_in, factors_out=factors_out, decay_rates=decay_rates, norm_gain=norm_gain, reward_dir=reward_dir)


noise_scale = 0.25
norm_eps = 1e-06
spread_eps = 1e-05

def recurrence(inputs, decay):
    time_major = jnp.moveaxis(inputs, 2, 0)

    def advance(carried, column):
        carried = decay * carried + (1.0 - decay) * column
        return (carried, carried)
    initial = jnp.zeros(time_major.shape[1:], jnp.float32)
    _, states = lax.scan(advance, initial, time_major)
    return jnp.moveaxis(states, 0, 2)

def reference(token_ids, fitness_ranks, embedding, mix_weights, factors_in, factors_out, decay_rates, norm_gain, reward_dir):
    block_width = D // N_MP
    coef = noise_scale * (D * RANK) ** (-0.5)
    hidden = jnp.take(embedding, token_ids, axis=0)
    shape_full = hidden.shape
    for layer_idx in range(LAYERS):
        base_mix = jnp.zeros((MEMBERS * SEQS * STEPS, D), jnp.float32)
        for shard_idx in range(N_MP):
            portion = hidden[..., shard_idx * block_width:(shard_idx + 1) * block_width].reshape(-1, block_width)
            rows_w = mix_weights[layer_idx, shard_idx * block_width:(shard_idx + 1) * block_width, :]
            partial_value = jnp.dot(portion, rows_w, preferred_element_type=jnp.float32).astype(jnp.bfloat16)
            partial_value = lax.optimization_barrier(partial_value)
            base_mix = base_mix + partial_value.astype(jnp.float32)
        base_mix = base_mix.reshape(shape_full)
        low_rank = jnp.einsum('mstd,mrd->mstr', hidden.astype(jnp.float32), factors_in[layer_idx].astype(jnp.float32))
        correction = jnp.einsum('mstr,mrd->mstd', low_rank, factors_out[layer_idx].astype(jnp.float32), precision=lax.Precision.HIGHEST)
        mixed = base_mix + coef * correction
        states = recurrence(mixed, decay_rates[layer_idx])
        mean_sq = lax.optimization_barrier(jnp.mean(states * states, axis=3, keepdims=True))
        norm_scale = lax.rsqrt(mean_sq + norm_eps)
        hidden = (hidden.astype(jnp.float32) + states * norm_scale * norm_gain[layer_idx]).astype(jnp.bfloat16)
    final_features = hidden[:, :, STEPS - 1, :]
    dots = jnp.einsum('mstd,d->mst', hidden.astype(jnp.float32), reward_dir, precision=lax.Precision.HIGHEST)
    scores = lax.optimization_barrier(jnp.mean(dots, axis=2)) * D ** (-0.5)
    shares = fitness_ranks.astype(jnp.float32) / MEMBERS
    rank_mean = jnp.mean(shares)
    rank_spread = jnp.mean((shares - rank_mean) * (shares - rank_mean)) + spread_eps
    shaped = (shares - rank_mean) * lax.rsqrt(rank_spread)
    deltas = []
    for layer_idx in range(LAYERS):
        weighted = (factors_in[layer_idx].astype(jnp.float32) * shaped[:, None, None]).astype(jnp.bfloat16)
        outer = factors_out[layer_idx]
        delta = jnp.dot(weighted.reshape(-1, D).T, outer.reshape(-1, D), preferred_element_type=jnp.float32)
        deltas.append(delta * (MEMBERS * RANK) ** (-0.5))
    weight_step = jnp.stack(deltas, axis=0)
    return (final_features, scores, weight_step)
```

```python
import jax
import jax.numpy as jnp
from jax import lax
from jax.sharding import PartitionSpec as P

noise_scale = 0.25
norm_eps = 1e-06
spread_eps = 1e-05


def recurrence(inputs, decay):
    carried = jnp.zeros(inputs.shape[1:], jnp.float32)
    states = []
    for step in range(inputs.shape[0]):
        carried = decay * carried + (1.0 - decay) * inputs[step]
        states.append(carried)
    return jnp.stack(states, axis=0)


def mixed_inputs(hidden, weight_rows):
    flat = hidden.reshape(-1, hidden.shape[-1])
    partial_value = jnp.dot(flat, weight_rows, preferred_element_type=jnp.float32)
    summed = lax.psum_scatter(
        partial_value.astype(jnp.bfloat16), "mp", scatter_dimension=1, tiled=True
    ).astype(jnp.float32)
    return summed


def project_rank(hidden, factor_rows):
    return jnp.einsum("tmsd,mrd->tmsr", hidden, factor_rows, preferred_element_type=jnp.float32)


def shards(
    token_ids,
    fitness_ranks,
    embedding,
    mix_weights,
    factors_in,
    factors_out,
    decay_rates,
    norm_gain,
    reward_dir,
):
    members, seq_count, step_count = token_ids.shape
    local_width = embedding.shape[1]
    vocab_size = embedding.shape[0]
    layers = mix_weights.shape[0]
    full_width = mix_weights.shape[2]
    rank_count = factors_in.shape[2]
    pop_count = lax.axis_size("pop")
    members_all = members * pop_count
    coef = noise_scale * (full_width * rank_count) ** (-0.5)
    position = lax.axis_index("mp")
    outputs_local = lax.dynamic_slice_in_dim(
        factors_out, position * local_width, local_width, 3
    ).astype(jnp.float32)
    onehot = (
        jnp.moveaxis(token_ids, 2, 0).reshape(-1)[:, None] == jnp.arange(vocab_size, dtype=jnp.int32)[None, :]
    ).astype(jnp.bfloat16)
    hidden = jnp.dot(onehot, embedding, preferred_element_type=jnp.float32).astype(jnp.bfloat16)
    hidden = hidden.reshape(step_count, members, seq_count, local_width)
    for layer_idx in range(layers):
        if layer_idx == 0:
            table = mixed_inputs(embedding, mix_weights[0])
            top = table.astype(jnp.bfloat16)
            rest = (table - top.astype(jnp.float32)).astype(jnp.bfloat16)
            base_mix = jnp.dot(onehot, top, preferred_element_type=jnp.float32) + jnp.dot(
                onehot, rest, preferred_element_type=jnp.float32
            )
        else:
            base_mix = mixed_inputs(hidden, mix_weights[layer_idx])
        base_mix = base_mix.reshape(hidden.shape)
        low_rank = lax.psum(project_rank(hidden, factors_in[layer_idx]), "mp")
        correction = jnp.einsum(
            "tmsr,mrd->tmsd", low_rank, outputs_local[layer_idx], precision=lax.Precision.HIGHEST
        )
        states = recurrence(base_mix + coef * correction, decay_rates[layer_idx])
        squares = lax.psum(jnp.sum(states * states, axis=3), "mp")
        norm_scale = lax.rsqrt(squares / full_width + norm_eps)
        hidden = (
            hidden.astype(jnp.float32) + states * norm_scale[..., None] * norm_gain[layer_idx]
        ).astype(jnp.bfloat16)
    dots_local = jnp.einsum(
        "tmsd,d->tms", hidden.astype(jnp.float32), reward_dir, precision=lax.Precision.HIGHEST
    )
    reward_terms = lax.psum(dots_local, "mp")
    final_features = hidden[step_count - 1]
    scores = jnp.mean(reward_terms, axis=0) * full_width ** (-0.5)
    ranks_every = lax.all_gather(fitness_ranks, "pop", axis=0, tiled=True)
    shares_all = ranks_every.astype(jnp.float32) / members_all
    rank_mean = jnp.mean(shares_all)
    rank_spread = jnp.mean((shares_all - rank_mean) * (shares_all - rank_mean)) + spread_eps
    shaped_all = (shares_all - rank_mean) * lax.rsqrt(rank_spread)
    columns = lax.all_to_all(factors_out, "pop", split_axis=3, concat_axis=1, tiled=True)
    weighted = (
        lax.all_gather(factors_in, "pop", axis=1, tiled=True).astype(jnp.float32)
        * shaped_all[None, :, None, None]
    ).astype(jnp.bfloat16)
    weight_delta = jnp.einsum(
        "lmri,lmro->lio", weighted, columns, preferred_element_type=jnp.float32
    )
    weight_step = weight_delta * (members_all * rank_count) ** (-0.5)
    return (final_features, scores, weight_step)


def solution(mesh):
    return jax.shard_map(
        shards,
        mesh=mesh,
        in_specs=(
            P("pop", None, None),
            P("pop"),
            P(None, "mp"),
            P(None, "mp", None),
            P(None, "pop", None, "mp"),
            P(None, "pop", None, None),
            P(None, "mp"),
            P(None, "mp"),
            P("mp"),
        ),
        out_specs=(P("pop", None, "mp"), P("pop", None), P(None, "mp", "pop")),
        check_vma=False,
    )
```

```python
import functools

import jax
import jax.numpy as jnp
from jax import lax
from jax.experimental import pallas as pl
from jax.experimental.pallas import tpu as pltpu
from jax.sharding import PartitionSpec as P

noise_scale = 0.25
norm_eps = 1e-06
spread_eps = 1e-05
lanes = 128
f32, bf16 = jnp.float32, jnp.bfloat16


def policy_kernel(
    dims,
    onehot_ref,
    embed_ref,
    mix_ref,
    fin_ref,
    fout_ref,
    ranks_ref,
    decay_ref,
    gain_ref,
    reward_ref,
    final_ref,
    score_ref,
    gin_ref,
    gout_ref,
    granks_ref,
    weights,
    own_pair,
    got_pair,
    own_cross,
    got_cross,
    states,
    hidden,
    table,
    small,
    marks,
    weight_sem,
    pair_send,
    pair_recv,
    cross_send,
    cross_recv,
    small_send,
    small_recv,
    mark_send,
    mark_recv,
    pop_send,
    pop_recv,
    self_sem,
):
    pop, chunks, group, steps, member_rows, seqs, rank, width, full, coef = dims
    rows = group * steps
    vocab = embed_ref.shape[0]
    local = fin_ref.shape[1]
    columns = gout_ref.shape[2]
    mine = lax.axis_index("pop")
    me = lax.axis_index("mp")
    side, core = me // 2, me % 2
    mate = side * 2 + (1 - core)
    cross = (1 - side) * 2 + core
    diagonal = (1 - side) * 2 + (1 - core)
    others = (mate, cross, diagonal)
    blocks = (diagonal, cross, mate, me)

    def peer(q, j):
        return {"pop": q, "mp": j}

    def remote(src, dst, send, recv, q, j):
        return pltpu.make_async_remote_copy(
            src_ref=src,
            dst_ref=dst,
            send_sem=send,
            recv_sem=recv,
            device_id=peer(q, j),
            device_id_type=pl.DeviceIdType.MESH,
        )

    def weight_copy(layer, slot):
        start = pl.multiple_of(blocks[slot] * width, lanes)
        return pltpu.make_async_copy(
            mix_ref.at[layer, :, pl.ds(start, width)],
            weights.at[layer, slot],
            weight_sem.at[layer, slot],
        )

    for layer in range(2):
        for slot in range(4):
            weight_copy(layer, slot).start()

    barrier = pltpu.get_barrier_semaphore()
    for other in others:
        pl.semaphore_signal(
            barrier, inc=1, device_id=peer(mine, other), device_id_type=pl.DeviceIdType.MESH
        )

    def greet(hop, carry):
        pl.semaphore_signal(
            barrier,
            inc=1,
            device_id=peer(lax.rem(mine + hop, pop), me),
            device_id_type=pl.DeviceIdType.MESH,
        )
        return carry

    lax.fori_loop(1, pop, greet, 0)
    pl.semaphore_wait(barrier, 3 + pop - 1)

    def pop_copies(hop, source):
        target = lax.rem(mine + hop, pop)
        at = pl.multiple_of(source * local, local)
        cols = pl.multiple_of(target * columns, lanes)
        return (
            remote(
                fin_ref,
                gin_ref.at[:, pl.ds(at, local), :],
                pop_send.at[0, hop],
                pop_recv.at[0, hop],
                target,
                me,
            ),
            remote(
                fout_ref.at[:, :, pl.ds(cols, columns)],
                gout_ref.at[:, pl.ds(at, local), :],
                pop_send.at[1, hop],
                pop_recv.at[1, hop],
                target,
                me,
            ),
            remote(
                ranks_ref,
                granks_ref.at[source],
                pop_send.at[2, hop],
                pop_recv.at[2, hop],
                target,
                me,
            ),
        )

    def self_copies():
        at = pl.multiple_of(mine * local, local)
        cols = pl.multiple_of(mine * columns, lanes)
        return (
            pltpu.make_async_copy(fin_ref, gin_ref.at[:, pl.ds(at, local), :], self_sem.at[0]),
            pltpu.make_async_copy(
                fout_ref.at[:, :, pl.ds(cols, columns)],
                gout_ref.at[:, pl.ds(at, local), :],
                self_sem.at[1],
            ),
            pltpu.make_async_copy(ranks_ref, granks_ref.at[mine], self_sem.at[2]),
        )

    def send_pop(hop, carry):
        for copy in pop_copies(hop, mine):
            copy.start()
        return carry

    def small_copy(kind, g, r):
        return remote(
            small.at[kind, g, 0],
            small.at[kind, g, r + 1],
            small_send.at[kind, g, r],
            small_recv.at[kind, g, r],
            mine,
            others[r],
        )

    def small_start(kind, g, value):
        small[kind, g, 0] = value
        for r in range(3):
            small_copy(kind, g, r).start()

    def small_sum(kind, g):
        for r in range(3):
            small_copy(kind, g, r).wait_recv()
        return (small[kind, g, 0] + small[kind, g, 1]) + (small[kind, g, 2] + small[kind, g, 3])

    def pair_copy(k, slot):
        return remote(
            own_pair.at[k, slot],
            got_pair.at[k, slot],
            pair_send.at[k, slot],
            pair_recv.at[k, slot],
            mine,
            mate,
        )

    def cross_copy(k):
        return remote(
            own_cross.at[k], got_cross.at[k], cross_send.at[k], cross_recv.at[k], mine, cross
        )

    def mark_copy(g, r):
        return remote(
            marks.at[g, 0],
            marks.at[g, r + 1],
            mark_send.at[g, r],
            mark_recv.at[g, r],
            mine,
            others[r],
        )

    def exchange(k, read, count, layer, before):
        def product(slot):
            before(slot)
            return jnp.dot(read(), weights[layer, slot], preferred_element_type=f32).astype(bf16)

        own_pair[k, 0, :count] = product(0)
        pair_copy(k, 0).start()
        own_cross[k, :count] = product(1)
        pair_copy(k, 0).wait_recv()
        own_cross[k, :count] = (
            own_cross[k, :count].astype(f32) + got_pair[k, 0, :count].astype(f32)
        ).astype(bf16)
        cross_copy(k).start()
        own_pair[k, 1, :count] = product(2)
        pair_copy(k, 1).start()
        return product(3).astype(f32)

    def received(k, count):
        pair_copy(k, 1).wait_recv()
        cross_copy(k).wait_recv()
        return got_pair[k, 1, :count].astype(f32) + got_cross[k, :count].astype(f32)

    factor_rows = member_rows * rank
    mask = (lax.broadcasted_iota(jnp.int32, (factor_rows, rows), 0) // rank) == (
        (lax.broadcasted_iota(jnp.int32, (factor_rows, rows), 1) % group) // seqs
    )

    def factor_slice(ref, layer, g, start, size):
        at = pl.multiple_of(g * factor_rows, factor_rows)
        return ref[layer, pl.ds(at, factor_rows), pl.ds(start, size)]

    def low_start(layer, g, features):
        local_low = lax.dot_general(
            factor_slice(fin_ref, layer, g, 0, width),
            features,
            (((1,), (1,)), ((), ())),
            preferred_element_type=f32,
        )
        local_low = jnp.where(mask, local_low, 0.0)
        packed = local_low[:8]
        for at in range(8, factor_rows, 8):
            packed = packed + local_low[at : at + 8]
        small_start(layer, g, packed)

    def correction(layer, g):
        packed = small_sum(layer, g)
        low = jnp.concatenate([packed] * (factor_rows // 8), axis=0)
        low = jnp.where(mask, low, 0.0) * coef
        top = low.astype(bf16).astype(f32)
        blank = jnp.zeros((lanes - 2 * factor_rows, rows), f32)
        stacked = jnp.concatenate([top, low - top, blank], axis=0)
        factor = factor_slice(fout_ref, layer, g, pl.multiple_of(me * width, lanes), width)
        right = jnp.concatenate(
            [factor, factor, jnp.zeros((lanes - 2 * factor_rows, width), bf16)], axis=0
        )
        return jnp.dot(stacked.T.astype(bf16), right, preferred_element_type=f32)

    def recur(layer, g):
        decay = decay_ref[layer : layer + 1, :]
        kept = 1.0 - decay

        def advance(t, carried):
            at = pl.ds(pl.multiple_of(t * group, group), group)
            carried = decay * carried + kept * states[g, at, :]
            states[g, at, :] = carried
            return carried

        lax.fori_loop(0, steps, advance, jnp.zeros((group, width), f32), unroll=2)

        part = states[g, :, 0:lanes]
        total = part * part
        for t in range(1, width // lanes):
            part = states[g, :, t * lanes : (t + 1) * lanes]
            total = total + part * part
        total = total.T
        packed = total[:8]
        for at in range(8, lanes, 8):
            packed = packed + total[at : at + 8]
        small_start(2 + layer, g, packed)

    def normed(layer, g):
        squares = jnp.sum(small_sum(2 + layer, g), axis=0, keepdims=True)
        scale = lax.rsqrt(squares / full + norm_eps)
        scale = jnp.broadcast_to(scale, (lanes, rows)).T
        scale = jnp.concatenate([scale] * (width // lanes), axis=1)
        gain = gain_ref[layer : layer + 1, :]
        return (hidden[g].astype(f32) + states[g] * scale * gain).astype(bf16)

    first = exchange(
        0, lambda: embed_ref[...], vocab, 0, lambda slot: weight_copy(0, slot).wait()
    )
    lax.fori_loop(1, pop, send_pop, 0)
    for copy in self_copies():
        copy.start()

    def begin(g, carry):
        features = jnp.dot(onehot_ref[g], embed_ref[...], preferred_element_type=f32).astype(bf16)
        hidden[g] = features
        low_start(0, g, features)
        return carry

    lax.fori_loop(0, chunks, begin, 0)
    for slot in range(4):
        weight_copy(1, slot).wait()
    whole = first + received(0, vocab)
    top = whole.astype(bf16)
    table[0] = top
    table[1] = (whole - top.astype(f32)).astype(bf16)

    def layer_zero(g, carry):
        picks = onehot_ref[g]
        states[g] = (
            jnp.dot(picks, table[0], preferred_element_type=f32)
            + jnp.dot(picks, table[1], preferred_element_type=f32)
            + correction(0, g)
        )
        recur(0, g)
        return carry

    lax.fori_loop(0, chunks, layer_zero, 0)

    def between(g, carry):
        hidden[g] = normed(0, g)
        states[g] = exchange(1 + g, lambda: hidden[g], rows, 1, lambda slot: None)
        low_start(1, g, hidden[g])
        return carry

    lax.fori_loop(0, chunks, between, 0)

    def layer_one(g, carry):
        states[g] = states[g] + received(1 + g, rows) + correction(1, g)
        recur(1, g)
        return carry

    def finish(g, carry):
        last = normed(1, g)
        at = pl.ds(pl.multiple_of(g * group, group), group)
        final_ref[at, :] = last[rows - group :]
        total = last[:group].astype(f32)
        for t in range(1, steps):
            total = total + last[t * group : (t + 1) * group].astype(f32)
        total = total * reward_ref[...]
        packed = total[:, :lanes]
        for t in range(1, width // lanes):
            packed = packed + total[:, t * lanes : (t + 1) * lanes]
        marks[g, 0] = packed
        for r in range(3):
            mark_copy(g, r).start()
        return carry

    lax.fori_loop(0, chunks, lambda g, carry: finish(g, layer_one(g, carry)), 0)

    def collect(g, carry):
        for r in range(3):
            mark_copy(g, r).wait_recv()
        at = pl.ds(pl.multiple_of(g * group, group), group)
        score_ref[at, :] = (marks[g, 0] + marks[g, 1]) + (marks[g, 2] + marks[g, 3])
        for r in range(3):
            mark_copy(g, r).wait_send()
            for kind in range(4):
                small_copy(kind, g, r).wait_send()
        return carry

    lax.fori_loop(0, chunks, collect, 0)

    def drain(k, carry):
        pair_copy(k, 0).wait_send()
        pair_copy(k, 1).wait_send()
        cross_copy(k).wait_send()
        return carry

    lax.fori_loop(0, chunks + 1, drain, 0)

    def drain_pop(hop, carry):
        for copy in pop_copies(hop, lax.rem(mine + pop - hop, pop)):
            copy.wait_recv()
        for copy in pop_copies(hop, mine):
            copy.wait_send()
        return carry

    lax.fori_loop(1, pop, drain_pop, 0)
    for copy in self_copies():
        copy.wait()


def shards(
    token_ids,
    fitness_ranks,
    embedding,
    mix_weights,
    factors_in,
    factors_out,
    decay_rates,
    norm_gain,
    reward_dir,
):
    members, seqs, steps = token_ids.shape
    vocab, width = embedding.shape
    layers, _, full = mix_weights.shape
    rank = factors_in.shape[2]
    pop = lax.axis_size("pop")
    members_all = members * pop
    coef = noise_scale * (full * rank) ** (-0.5)
    columns = full // pop
    member_rows = 16 // seqs
    chunks = members // member_rows
    group = member_rows * seqs
    rows = group * steps
    local = members * rank
    ids = token_ids.reshape(chunks, member_rows, seqs, steps)
    ids = jnp.transpose(ids, (0, 3, 1, 2)).reshape(chunks, rows)
    onehot = (ids[:, :, None] == jnp.arange(vocab, dtype=jnp.int32)).astype(bf16)
    ranks = jnp.zeros((8, lanes), jnp.int32)
    ranks = lax.dynamic_update_slice(ranks, fitness_ranks[None, :], (0, 0))
    dims = (pop, chunks, group, steps, member_rows, seqs, rank, width, full, coef)
    vmem = pl.BlockSpec(memory_space=pltpu.VMEM)
    hbm = pl.BlockSpec(memory_space=pl.ANY)
    most = max(rows, vocab)
    phases = chunks + 1
    dma = pltpu.SemaphoreType.DMA
    final, marks, gin, gout, granks = pl.pallas_call(
        functools.partial(policy_kernel, dims),
        out_shape=(
            jax.ShapeDtypeStruct((members * seqs, width), bf16),
            jax.ShapeDtypeStruct((members * seqs, lanes), f32),
            jax.ShapeDtypeStruct((layers, pop * local, width), bf16),
            jax.ShapeDtypeStruct((layers, pop * local, columns), bf16),
            jax.ShapeDtypeStruct((pop, 8, lanes), jnp.int32),
        ),
        in_specs=[vmem, vmem, hbm, vmem, vmem, vmem, vmem, vmem, vmem],
        out_specs=(vmem, vmem, hbm, hbm, hbm),
        scratch_shapes=[
            pltpu.VMEM((layers, 4, width, width), bf16),
            pltpu.VMEM((phases, 2, most, width), bf16),
            pltpu.VMEM((phases, 2, most, width), bf16),
            pltpu.VMEM((phases, most, width), bf16),
            pltpu.VMEM((phases, most, width), bf16),
            pltpu.VMEM((chunks, rows, width), f32),
            pltpu.VMEM((chunks, rows, width), bf16),
            pltpu.VMEM((2, vocab, width), bf16),
            pltpu.VMEM((4, chunks, 4, 8, rows), f32),
            pltpu.VMEM((chunks, 4, group, lanes), f32),
            dma((layers, 4)),
            dma((phases, 2)),
            dma((phases, 2)),
            dma((phases,)),
            dma((phases,)),
            dma((4, chunks, 3)),
            dma((4, chunks, 3)),
            dma((chunks, 3)),
            dma((chunks, 3)),
            dma((3, pop)),
            dma((3, pop)),
            dma((3,)),
        ],
        compiler_params=pltpu.CompilerParams(
            collective_id=0, has_side_effects=True, vmem_limit_bytes=60 * 1024 * 1024
        ),
    )(
        onehot,
        embedding,
        mix_weights,
        factors_in.reshape(layers, local, width),
        factors_out.reshape(layers, local, full),
        ranks,
        decay_rates,
        norm_gain,
        reward_dir.reshape(1, width),
    )
    final_features = final.reshape(members, seqs, width)
    scores = jnp.sum(marks, axis=1).reshape(members, seqs) * (full ** (-0.5) / steps)
    ranks_every = granks[:, 0, :members].reshape(-1)
    shares_all = ranks_every.astype(f32) / members_all
    rank_mean = jnp.mean(shares_all)
    rank_spread = jnp.mean((shares_all - rank_mean) * (shares_all - rank_mean)) + spread_eps
    shaped_all = (shares_all - rank_mean) * lax.rsqrt(rank_spread)
    shaped_rows = jnp.repeat(shaped_all, rank)
    weighted = (gin.astype(f32) * shaped_rows[None, :, None]).astype(bf16)
    weight_delta = jnp.einsum("lki,lko->lio", weighted, gout, preferred_element_type=f32)
    weight_step = weight_delta * (members_all * rank) ** (-0.5)
    return (final_features, scores, weight_step)


def solution(mesh):
    return jax.shard_map(
        shards,
        mesh=mesh,
        in_specs=(
            P("pop", None, None),
            P("pop"),
            P(None, "mp"),
            P(None, "mp", None),
            P(None, "pop", None, "mp"),
            P(None, "pop", None, None),
            P(None, "mp"),
            P(None, "mp"),
            P("mp"),
        ),
        out_specs=(P("pop", None, "mp"), P("pop", None), P(None, "mp", "pop")),
        check_vma=False,
    )
```

```python
import functools

import jax
import jax.numpy as jnp
from jax import lax
from jax.experimental import pallas as pl
from jax.experimental.pallas import tpu as pltpu
from jax.sharding import PartitionSpec as P

noise_scale = 0.25
norm_eps = 1e-06
spread_eps = 1e-05
lanes = 128
f32, bf16 = jnp.float32, jnp.bfloat16


def policy_kernel(
    dims,
    onehot_ref,
    embed_ref,
    mix_ref,
    fin_raw,
    fout_raw,
    ranks_smem,
    decay_ref,
    gain_ref,
    reward_ref,
    final_ref,
    score_ref,
    gin_ref,
    gout_ref,
    weights,
    own_pair,
    got_pair,
    own_cross,
    got_cross,
    states,
    hidden,
    fin_ref,
    fout_ref,
    scaled,
    ranks,
    granks_ref,
    lows,
    squares,
    small,
    marks,
    weight_sem,
    pair_send,
    pair_recv,
    cross_send,
    cross_recv,
    small_send,
    small_recv,
    mark_send,
    mark_recv,
    pop_send,
    pop_recv,
    self_sem,
):
    pop, chunks, group, steps, member_rows, seqs, rank, width, full, coef = dims
    parts = pair_send.shape[2]
    piece = width // parts
    halves = [slice(p * piece, (p + 1) * piece) for p in range(parts)]
    rows = group * steps
    vocab = embed_ref.shape[0]
    local = fin_ref.shape[1]
    columns = gout_ref.shape[2]
    mine = lax.axis_index("pop")
    me = lax.axis_index("mp")
    side, core = me // 2, me % 2
    mate = side * 2 + (1 - core)
    cross = (1 - side) * 2 + core
    diagonal = (1 - side) * 2 + (1 - core)
    others = (mate, cross, diagonal)
    blocks = (diagonal, cross, mate, me)

    def peer(q, j):
        return {"pop": q, "mp": j}

    def remote(src, dst, send, recv, q, j):
        return pltpu.make_async_remote_copy(
            src_ref=src,
            dst_ref=dst,
            send_sem=send,
            recv_sem=recv,
            device_id=peer(q, j),
            device_id_type=pl.DeviceIdType.MESH,
        )

    def weight_copy(layer, slot):
        start = pl.multiple_of(blocks[slot] * width, lanes)
        return pltpu.make_async_copy(
            mix_ref.at[layer, :, pl.ds(start, width)],
            weights.at[layer, slot],
            weight_sem.at[layer, slot],
        )

    for layer in range(2):
        for slot in range(4):
            weight_copy(layer, slot).start()

    barrier = pltpu.get_barrier_semaphore()
    for other in others:
        pl.semaphore_signal(
            barrier, inc=1, device_id=peer(mine, other), device_id_type=pl.DeviceIdType.MESH
        )

    def greet(hop, carry):
        pl.semaphore_signal(
            barrier,
            inc=1,
            device_id=peer(lax.rem(mine + hop, pop), me),
            device_id_type=pl.DeviceIdType.MESH,
        )
        return carry

    lax.fori_loop(1, pop, greet, 0)
    pl.semaphore_wait(barrier, 3 + pop - 1)

    members = ranks_smem.shape[0]
    members_all = members * pop

    def rank_copy(hop, source):
        return remote(
            ranks,
            granks_ref.at[source],
            pop_send.at[2, hop],
            pop_recv.at[2, hop],
            lax.rem(mine + hop, pop),
            me,
        )

    def out_copy(hop, source):
        target = lax.rem(mine + hop, pop)
        at = pl.multiple_of(source * local, local)
        cols = pl.multiple_of(target * columns, lanes)
        return remote(
            fout_ref.at[:, :, pl.ds(cols, columns)],
            gout_ref.at[:, pl.ds(at, local), :],
            pop_send.at[1, hop],
            pop_recv.at[1, hop],
            target,
            me,
        )

    def in_copy(hop, source):
        at = pl.multiple_of(source * local, local)
        return remote(
            scaled,
            gin_ref.at[:, pl.ds(at, local), :],
            pop_send.at[0, hop],
            pop_recv.at[0, hop],
            lax.rem(mine + hop, pop),
            me,
        )

    def self_copies():
        at = pl.multiple_of(mine * local, local)
        cols = pl.multiple_of(mine * columns, lanes)
        return (
            pltpu.make_async_copy(scaled, gin_ref.at[:, pl.ds(at, local), :], self_sem.at[0]),
            pltpu.make_async_copy(
                fout_ref.at[:, :, pl.ds(cols, columns)],
                gout_ref.at[:, pl.ds(at, local), :],
                self_sem.at[1],
            ),
        )

    def send_with(make):
        def send(hop, carry):
            make(hop, mine).start()
            return carry

        lax.fori_loop(1, pop, send, 0)

    def rank_block(shape, axis, repeats):
        index = lax.broadcasted_iota(jnp.int32, shape, axis)
        block = jnp.zeros(shape, jnp.int32)
        for m in range(members):
            block = jnp.where(index // repeats == m, ranks_smem[m], block)
        return block

    ranks[...] = rank_block((8, lanes), 1, 1)
    send_with(rank_copy)
    granks_ref[mine] = ranks[...]

    def unpack(g, carry):
        at = pl.ds(pl.multiple_of(g * member_rows * rank, member_rows * rank), member_rows * rank)
        for layer in range(2):
            for raw, ref in ((fin_raw, fin_ref), (fout_raw, fout_ref)):
                ref[layer, at, :] = jnp.concatenate(
                    [raw[layer, g * member_rows + m].astype(f32) for m in range(member_rows)],
                    axis=0,
                ).astype(bf16)
        return carry

    def shape_ranks():
        def arrived(hop, carry):
            rank_copy(hop, lax.rem(mine + pop - hop, pop)).wait_recv()
            return carry

        lax.fori_loop(1, pop, arrived, 0)
        full_block = (pop, 8, lanes)
        kept = (lax.broadcasted_iota(jnp.int32, full_block, 1) == 0) & (
            lax.broadcasted_iota(jnp.int32, full_block, 2) < members
        )
        shares = jnp.where(kept, granks_ref[...].astype(f32) / members_all, 0.0)

        def mean_of(value):
            value = jnp.sum(value, axis=0)
            value = jnp.sum(value, axis=0, keepdims=True)
            return jnp.sum(value, axis=1, keepdims=True) / members_all

        rank_mean = mean_of(shares)
        apart = jnp.where(kept, shares - rank_mean[None], 0.0)
        spread = mean_of(apart * apart) + spread_eps
        own = rank_block((local, lanes), 0, rank).astype(f32) / members_all
        shaped = (own - rank_mean) * lax.rsqrt(spread)
        shaped = jnp.concatenate([shaped] * (width // lanes), axis=1)
        for layer in range(2):
            scaled[layer] = (fin_ref[layer].astype(f32) * shaped).astype(bf16)

    def small_copy(kind, g, r):
        return remote(
            small.at[kind, g, 0],
            small.at[kind, g, r + 1],
            small_send.at[kind, g, r],
            small_recv.at[kind, g, r],
            mine,
            others[r],
        )

    def small_start(kind, g, value):
        small[kind, g, 0] = value
        for r in range(3):
            small_copy(kind, g, r).start()

    def small_sum(kind, g):
        for r in range(3):
            small_copy(kind, g, r).wait_recv()
        return (small[kind, g, 0] + small[kind, g, 1]) + (small[kind, g, 2] + small[kind, g, 3])

    def pair_copy(k, slot, p):
        return remote(
            own_pair.at[k, slot, p],
            got_pair.at[k, slot, p],
            pair_send.at[k, slot, p],
            pair_recv.at[k, slot, p],
            mine,
            mate,
        )

    def cross_copy(k, p):
        return remote(
            own_cross.at[k, p],
            got_cross.at[k, p],
            cross_send.at[k, p],
            cross_recv.at[k, p],
            mine,
            cross,
        )

    def mark_copy(g, r):
        return remote(
            marks.at[g, 0],
            marks.at[g, r + 1],
            mark_send.at[g, r],
            mark_recv.at[g, r],
            mine,
            others[r],
        )

    def exchange(k, read, count, layer, before, put):
        def product(slot, p):
            return jnp.dot(
                read(), weights[layer, slot, :, halves[p]], preferred_element_type=f32
            ).astype(bf16)

        before(0)
        for p in range(parts):
            own_pair[k, 0, p, :count] = product(0, p)
            pair_copy(k, 0, p).start()
        before(1)
        for p in range(parts):
            value = product(1, p).astype(f32)
            pair_copy(k, 0, p).wait_recv()
            own_cross[k, p, :count] = (value + got_pair[k, 0, p, :count].astype(f32)).astype(bf16)
            cross_copy(k, p).start()
        before(2)
        for p in range(parts):
            own_pair[k, 1, p, :count] = product(2, p)
            pair_copy(k, 1, p).start()
        before(3)
        for p in range(parts):
            put(halves[p], product(3, p).astype(f32))

    def received(k, count, p):
        pair_copy(k, 1, p).wait_recv()
        cross_copy(k, p).wait_recv()
        return got_pair[k, 1, p, :count].astype(f32) + got_cross[k, p, :count].astype(f32)

    factor_rows = member_rows * rank
    mask = (lax.broadcasted_iota(jnp.int32, (factor_rows, rows), 0) // rank) == (
        (lax.broadcasted_iota(jnp.int32, (factor_rows, rows), 1) % group) // seqs
    )

    def factor_slice(ref, layer, g, start, size):
        at = pl.multiple_of(g * factor_rows, factor_rows)
        return ref[layer, pl.ds(at, factor_rows), pl.ds(start, size)]

    def low_start(layer, g, features):
        local_low = lax.dot_general(
            factor_slice(fin_ref, layer, g, 0, width),
            features,
            (((1,), (1,)), ((), ())),
            preferred_element_type=f32,
        )
        local_low = jnp.where(mask, local_low, 0.0)
        packed = local_low[:8]
        for at in range(8, factor_rows, 8):
            packed = packed + local_low[at : at + 8]
        small_start(layer, g, packed)

    def low_ready(layer, g):
        packed = small_sum(layer, g)
        low = jnp.concatenate([packed] * (factor_rows // 8), axis=0)
        low = jnp.where(mask, low, 0.0) * coef
        top = low.astype(bf16).astype(f32)
        blank = jnp.zeros((lanes - 2 * factor_rows, rows), f32)
        lows[g] = jnp.concatenate([top, low - top, blank], axis=0).T.astype(bf16)

    def correction(layer, g, p):
        start = pl.multiple_of(me * width + p * piece, lanes)
        factor = factor_slice(fout_ref, layer, g, start, piece)
        right = jnp.concatenate(
            [factor, factor, jnp.zeros((lanes - 2 * factor_rows, piece), bf16)], axis=0
        )
        return jnp.dot(lows[g], right, preferred_element_type=f32)

    def recur(layer, g, p, inputs):
        decay = decay_ref[layer : layer + 1, halves[p]]
        kept = 1.0 - decay
        carried = jnp.zeros((group, piece), f32)
        for t in range(steps):
            at = slice(t * group, (t + 1) * group)
            carried = decay * carried + kept * inputs[at]
            states[g, at, halves[p]] = carried
            powers = carried * carried
            total = powers[:, :lanes]
            for c in range(lanes, piece, lanes):
                total = total + powers[:, c : c + lanes]
            if p:
                total = total + squares[g, at, :]
            squares[g, at, :] = total

    def squares_start(layer, g):
        total = squares[g].T
        packed = total[:8]
        for at in range(8, lanes, 8):
            packed = packed + total[at : at + 8]
        small_start(2 + layer, g, packed)

    def normed(layer, g):
        squares = jnp.sum(small_sum(2 + layer, g), axis=0, keepdims=True)
        scale = lax.rsqrt(squares / full + norm_eps)
        scale = jnp.broadcast_to(scale, (lanes, rows)).T
        scale = jnp.concatenate([scale] * (width // lanes), axis=1)
        gain = gain_ref[layer : layer + 1, :]
        return (hidden[g].astype(f32) + states[g, :rows] * scale * gain).astype(bf16)

    def put_first(cols, value):
        states[0, :vocab, cols] = value

    exchange(
        0,
        lambda: embed_ref[...],
        vocab,
        0,
        lambda slot: weight_copy(0, slot).wait(),
        put_first,
    )
    lax.fori_loop(0, chunks, unpack, 0)
    send_with(out_copy)

    def begin(g, carry):
        features = jnp.dot(onehot_ref[g], embed_ref[...], preferred_element_type=f32).astype(bf16)
        hidden[g] = features
        low_start(0, g, features)
        return carry

    lax.fori_loop(0, chunks, begin, 0)
    shape_ranks()
    send_with(in_copy)
    for copy in self_copies():
        copy.start()
    for slot in range(4):
        weight_copy(1, slot).wait()

    def low_zero(g, carry):
        low_ready(0, g)
        return carry

    lax.fori_loop(0, chunks, low_zero, 0)
    for p in range(parts):
        whole = states[0, :vocab, halves[p]] + received(0, vocab, p)
        top = whole.astype(bf16)
        rest = (whole - top.astype(f32)).astype(bf16)

        def layer_zero(g, carry, p=p, top=top, rest=rest):
            picks = onehot_ref[g]
            inputs = (
                jnp.dot(picks, top, preferred_element_type=f32)
                + jnp.dot(picks, rest, preferred_element_type=f32)
                + correction(0, g, p)
            )
            recur(0, g, p, inputs)
            if p == parts - 1:
                squares_start(0, g)
            return carry

        for g in range(chunks):
            layer_zero(g, 0)

    def between(g, carry):
        hidden[g] = normed(0, g)

        def put(cols, value):
            states[g, :rows, cols] = value

        exchange(1 + g, lambda: hidden[g], rows, 1, lambda slot: None, put)
        low_start(1, g, hidden[g])
        return carry

    lax.fori_loop(0, chunks, between, 0)

    def layer_one(g, carry):
        low_ready(1, g)
        for p in range(parts):
            inputs = states[g, :rows, halves[p]] + received(1 + g, rows, p) + correction(1, g, p)
            recur(1, g, p, inputs)
        squares_start(1, g)
        return carry

    def finish(g, carry):
        last = normed(1, g)
        at = pl.ds(pl.multiple_of(g * group, group), group)
        final_ref[at, :] = last[rows - group :]
        total = last[:group].astype(f32)
        for t in range(1, steps):
            total = total + last[t * group : (t + 1) * group].astype(f32)
        total = total * reward_ref[...]
        packed = total[:, :lanes]
        for t in range(1, width // lanes):
            packed = packed + total[:, t * lanes : (t + 1) * lanes]
        marks[g, 0] = packed
        for r in range(3):
            mark_copy(g, r).start()
        return carry

    lax.fori_loop(0, chunks, lambda g, carry: finish(g, layer_one(g, carry)), 0)

    def collect(g, carry):
        for r in range(3):
            mark_copy(g, r).wait_recv()
        at = pl.ds(pl.multiple_of(g * group, group), group)
        score_ref[at, :] = (marks[g, 0] + marks[g, 1]) + (marks[g, 2] + marks[g, 3])
        for r in range(3):
            mark_copy(g, r).wait_send()
            for kind in range(4):
                small_copy(kind, g, r).wait_send()
        return carry

    lax.fori_loop(0, chunks, collect, 0)

    def drain(k, carry):
        for p in range(parts):
            pair_copy(k, 0, p).wait_send()
            pair_copy(k, 1, p).wait_send()
            cross_copy(k, p).wait_send()
        return carry

    lax.fori_loop(0, chunks + 1, drain, 0)

    def drain_pop(hop, carry):
        source = lax.rem(mine + pop - hop, pop)
        in_copy(hop, source).wait_recv()
        out_copy(hop, source).wait_recv()
        for make in (rank_copy, in_copy, out_copy):
            make(hop, mine).wait_send()
        return carry

    lax.fori_loop(1, pop, drain_pop, 0)
    for copy in self_copies():
        copy.wait()


def shards(
    token_ids,
    fitness_ranks,
    embedding,
    mix_weights,
    factors_in,
    factors_out,
    decay_rates,
    norm_gain,
    reward_dir,
):
    members, seqs, steps = token_ids.shape
    vocab, width = embedding.shape
    layers, _, full = mix_weights.shape
    rank = factors_in.shape[2]
    pop = lax.axis_size("pop")
    members_all = members * pop
    coef = noise_scale * (full * rank) ** (-0.5)
    columns = full // pop
    member_rows = 16 // seqs
    chunks = members // member_rows
    group = member_rows * seqs
    rows = group * steps
    local = members * rank
    ids = token_ids.reshape(chunks, member_rows, seqs, steps)
    ids = jnp.transpose(ids, (0, 3, 1, 2)).reshape(chunks, rows)
    onehot = (ids[:, :, None] == jnp.arange(vocab, dtype=jnp.int32)).astype(bf16)
    dims = (pop, chunks, group, steps, member_rows, seqs, rank, width, full, coef)
    vmem = pl.BlockSpec(memory_space=pltpu.VMEM)
    smem = pl.BlockSpec(memory_space=pltpu.SMEM)
    hbm = pl.BlockSpec(memory_space=pl.ANY)
    most = max(rows, vocab)
    phases = chunks + 1
    parts = 4
    dma = pltpu.SemaphoreType.DMA
    final, marks, gin, gout = pl.pallas_call(
        functools.partial(policy_kernel, dims),
        out_shape=(
            jax.ShapeDtypeStruct((members * seqs, width), bf16),
            jax.ShapeDtypeStruct((members * seqs, lanes), f32),
            jax.ShapeDtypeStruct((layers, pop * local, width), bf16),
            jax.ShapeDtypeStruct((layers, pop * local, columns), bf16),
        ),
        in_specs=[vmem, vmem, hbm, vmem, vmem, smem, vmem, vmem, vmem],
        out_specs=(vmem, vmem, hbm, hbm),
        scratch_shapes=[
            pltpu.VMEM((layers, 4, width, width), bf16),
            pltpu.VMEM((phases, 2, parts, most, width // parts), bf16),
            pltpu.VMEM((phases, 2, parts, most, width // parts), bf16),
            pltpu.VMEM((phases, parts, most, width // parts), bf16),
            pltpu.VMEM((phases, parts, most, width // parts), bf16),
            pltpu.VMEM((chunks, most, width), f32),
            pltpu.VMEM((chunks, rows, width), bf16),
            pltpu.VMEM((layers, local, width), bf16),
            pltpu.VMEM((layers, local, full), bf16),
            pltpu.VMEM((layers, local, width), bf16),
            pltpu.VMEM((8, lanes), jnp.int32),
            pltpu.VMEM((pop, 8, lanes), jnp.int32),
            pltpu.VMEM((chunks, rows, lanes), bf16),
            pltpu.VMEM((chunks, rows, lanes), f32),
            pltpu.VMEM((4, chunks, 4, 8, rows), f32),
            pltpu.VMEM((chunks, 4, group, lanes), f32),
            dma((layers, 4)),
            dma((phases, 2, parts)),
            dma((phases, 2, parts)),
            dma((phases, parts)),
            dma((phases, parts)),
            dma((4, chunks, 3)),
            dma((4, chunks, 3)),
            dma((chunks, 3)),
            dma((chunks, 3)),
            dma((3, pop)),
            dma((3, pop)),
            dma((2,)),
        ],
        compiler_params=pltpu.CompilerParams(
            collective_id=0, has_side_effects=True, vmem_limit_bytes=60 * 1024 * 1024
        ),
    )(
        onehot,
        embedding,
        mix_weights,
        factors_in,
        factors_out,
        fitness_ranks,
        decay_rates,
        norm_gain,
        reward_dir.reshape(1, width),
    )
    final_features = final.reshape(members, seqs, width)
    scores = jnp.sum(marks, axis=1).reshape(members, seqs) * (full ** (-0.5) / steps)
    weight_delta = jnp.einsum("lki,lko->lio", gin, gout, preferred_element_type=f32)
    weight_step = weight_delta * (members_all * rank) ** (-0.5)
    return (final_features, scores, weight_step)


def solution(mesh):
    return jax.shard_map(
        shards,
        mesh=mesh,
        in_specs=(
            P("pop", None, None),
            P("pop"),
            P(None, "mp"),
            P(None, "mp", None),
            P(None, "pop", None, "mp"),
            P(None, "pop", None, None),
            P(None, "mp"),
            P(None, "mp"),
            P("mp"),
        ),
        out_specs=(P("pop", None, "mp"), P("pop", None), P(None, "mp", "pop")),
        check_vma=False,
    )
```

```python
import functools

import jax
import jax.numpy as jnp
from jax import lax
from jax.experimental import pallas as pl
from jax.experimental.pallas import tpu as pltpu
from jax.sharding import PartitionSpec as P

noise_scale = 0.25
norm_eps = 1e-06
spread_eps = 1e-05
lanes = 128
f32, bf16 = jnp.float32, jnp.bfloat16


def policy_kernel(
    dims,
    ids_ref,
    embed_ref,
    mix_ref,
    fin_raw,
    fout_hbm,
    ranks_smem,
    decay_ref,
    gain_ref,
    reward_ref,
    final_ref,
    score_ref,
    gin_ref,
    gout_ref,
    weights,
    own_pair,
    got_pair,
    own_cross,
    got_cross,
    states,
    hidden,
    onehot_ref,
    fout_raw,
    fin_ref,
    fout_ref,
    scaled,
    ranks,
    granks_ref,
    lows,
    squares,
    small,
    marks,
    weight_sem,
    pair_send,
    pair_recv,
    cross_send,
    cross_recv,
    small_send,
    small_recv,
    mark_send,
    mark_recv,
    pop_send,
    pop_recv,
    self_sem,
    load_sem,
):
    pop, chunks, group, steps, member_rows, seqs, rank, width, full, coef = dims
    parts = pair_send.shape[2]
    piece = width // parts
    halves = [slice(p * piece, (p + 1) * piece) for p in range(parts)]
    rows = group * steps
    vocab = embed_ref.shape[0]
    local = fin_ref.shape[1]
    columns = gout_ref.shape[2]
    mine = lax.axis_index("pop")
    me = lax.axis_index("mp")
    side, core = me // 2, me % 2
    mate = side * 2 + (1 - core)
    cross = (1 - side) * 2 + core
    diagonal = (1 - side) * 2 + (1 - core)
    others = (mate, cross, diagonal)
    blocks = (diagonal, cross, mate, me)

    def peer(q, j):
        return {"pop": q, "mp": j}

    def remote(src, dst, send, recv, q, j):
        return pltpu.make_async_remote_copy(
            src_ref=src,
            dst_ref=dst,
            send_sem=send,
            recv_sem=recv,
            device_id=peer(q, j),
            device_id_type=pl.DeviceIdType.MESH,
        )

    def weight_copy(layer, slot):
        start = pl.multiple_of(blocks[slot] * width, lanes)
        return pltpu.make_async_copy(
            mix_ref.at[layer, :, pl.ds(start, width)],
            weights.at[layer, slot],
            weight_sem.at[layer, slot],
        )

    for slot in range(4):
        weight_copy(0, slot).start()
    fout_load = pltpu.make_async_copy(fout_hbm, fout_raw, load_sem)
    fout_load.start()

    barrier = pltpu.get_barrier_semaphore()
    for other in others:
        pl.semaphore_signal(
            barrier, inc=1, device_id=peer(mine, other), device_id_type=pl.DeviceIdType.MESH
        )

    def greet(hop, carry):
        pl.semaphore_signal(
            barrier,
            inc=1,
            device_id=peer(lax.rem(mine + hop, pop), me),
            device_id_type=pl.DeviceIdType.MESH,
        )
        return carry

    lax.fori_loop(1, pop, greet, 0)
    pl.semaphore_wait(barrier, 3 + pop - 1)

    members = ranks_smem.shape[0]
    members_all = members * pop

    def rank_copy(hop, source):
        return remote(
            ranks,
            granks_ref.at[source],
            pop_send.at[2, hop],
            pop_recv.at[2, hop],
            lax.rem(mine + hop, pop),
            me,
        )

    def out_copy(hop, source):
        target = lax.rem(mine + hop, pop)
        at = pl.multiple_of(source * local, local)
        cols = pl.multiple_of(target * columns, lanes)
        return remote(
            fout_ref.at[:, :, pl.ds(cols, columns)],
            gout_ref.at[:, pl.ds(at, local), :],
            pop_send.at[1, hop],
            pop_recv.at[1, hop],
            target,
            me,
        )

    def in_copy(hop, source):
        at = pl.multiple_of(source * local, local)
        return remote(
            scaled,
            gin_ref.at[:, pl.ds(at, local), :],
            pop_send.at[0, hop],
            pop_recv.at[0, hop],
            lax.rem(mine + hop, pop),
            me,
        )

    def self_copies():
        at = pl.multiple_of(mine * local, local)
        cols = pl.multiple_of(mine * columns, lanes)
        return (
            pltpu.make_async_copy(scaled, gin_ref.at[:, pl.ds(at, local), :], self_sem.at[0]),
            pltpu.make_async_copy(
                fout_ref.at[:, :, pl.ds(cols, columns)],
                gout_ref.at[:, pl.ds(at, local), :],
                self_sem.at[1],
            ),
        )

    def send_with(make):
        def send(hop, carry):
            make(hop, mine).start()
            return carry

        lax.fori_loop(1, pop, send, 0)

    def rank_block(shape, axis, repeats):
        index = lax.broadcasted_iota(jnp.int32, shape, axis)
        block = jnp.zeros(shape, jnp.int32)
        for m in range(members):
            block = jnp.where(index // repeats == m, ranks_smem[m], block)
        return block

    ranks[...] = rank_block((8, lanes), 1, 1)
    send_with(rank_copy)
    granks_ref[mine] = ranks[...]

    def unpack(g, carry):
        at = pl.ds(pl.multiple_of(g * member_rows * rank, member_rows * rank), member_rows * rank)
        for layer in range(2):
            for raw, ref in ((fin_raw, fin_ref), (fout_raw, fout_ref)):
                ref[layer, at, :] = jnp.concatenate(
                    [raw[layer, g * member_rows + m].astype(f32) for m in range(member_rows)],
                    axis=0,
                ).astype(bf16)
        return carry

    def shape_ranks():
        def arrived(hop, carry):
            rank_copy(hop, lax.rem(mine + pop - hop, pop)).wait_recv()
            return carry

        lax.fori_loop(1, pop, arrived, 0)
        full_block = (pop, 8, lanes)
        kept = (lax.broadcasted_iota(jnp.int32, full_block, 1) == 0) & (
            lax.broadcasted_iota(jnp.int32, full_block, 2) < members
        )
        shares = jnp.where(kept, granks_ref[...].astype(f32) / members_all, 0.0)

        def mean_of(value):
            value = jnp.sum(value, axis=0)
            value = jnp.sum(value, axis=0, keepdims=True)
            return jnp.sum(value, axis=1, keepdims=True) / members_all

        rank_mean = mean_of(shares)
        apart = jnp.where(kept, shares - rank_mean[None], 0.0)
        spread = mean_of(apart * apart) + spread_eps
        own = rank_block((local, lanes), 0, rank).astype(f32) / members_all
        shaped = (own - rank_mean) * lax.rsqrt(spread)
        shaped = jnp.concatenate([shaped] * (width // lanes), axis=1)
        for layer in range(2):
            scaled[layer] = (fin_ref[layer].astype(f32) * shaped).astype(bf16)

    def small_copy(kind, g, r):
        return remote(
            small.at[kind, g, 0],
            small.at[kind, g, r + 1],
            small_send.at[kind, g, r],
            small_recv.at[kind, g, r],
            mine,
            others[r],
        )

    def small_start(kind, g, value):
        small[kind, g, 0] = value
        for r in range(3):
            small_copy(kind, g, r).start()

    def small_sum(kind, g):
        for r in range(3):
            small_copy(kind, g, r).wait_recv()
        return (small[kind, g, 0] + small[kind, g, 1]) + (small[kind, g, 2] + small[kind, g, 3])

    def pair_copy(k, slot, p):
        return remote(
            own_pair.at[k, slot, p],
            got_pair.at[k, slot, p],
            pair_send.at[k, slot, p],
            pair_recv.at[k, slot, p],
            mine,
            mate,
        )

    def cross_copy(k, p):
        return remote(
            own_cross.at[k, p],
            got_cross.at[k, p],
            cross_send.at[k, p],
            cross_recv.at[k, p],
            mine,
            cross,
        )

    def mark_copy(g, r):
        return remote(
            marks.at[g, 0],
            marks.at[g, r + 1],
            mark_send.at[g, r],
            mark_recv.at[g, r],
            mine,
            others[r],
        )

    def exchange(k, read, count, layer, before, put):
        def product(slot, p):
            return jnp.dot(
                read(), weights[layer, slot, :, halves[p]], preferred_element_type=f32
            ).astype(bf16)

        def summed(p):
            value = product(1, p).astype(f32)
            pair_copy(k, 0, p).wait_recv()
            own_cross[k, p, :count] = (value + got_pair[k, 0, p, :count].astype(f32)).astype(bf16)
            cross_copy(k, p).start()

        before(0)
        for p in range(parts):
            own_pair[k, 0, p, :count] = product(0, p)
            pair_copy(k, 0, p).start()
            if p == 1:
                before(1)
            if p:
                summed(p - 1)
        summed(parts - 1)
        before(2)
        for p in range(parts):
            own_pair[k, 1, p, :count] = product(2, p)
            pair_copy(k, 1, p).start()
        before(3)
        for p in range(parts):
            put(halves[p], product(3, p).astype(f32))

    def received(k, count, p):
        pair_copy(k, 1, p).wait_recv()
        cross_copy(k, p).wait_recv()
        return got_pair[k, 1, p, :count].astype(f32) + got_cross[k, p, :count].astype(f32)

    factor_rows = member_rows * rank
    mask = (lax.broadcasted_iota(jnp.int32, (factor_rows, rows), 0) // rank) == (
        (lax.broadcasted_iota(jnp.int32, (factor_rows, rows), 1) % group) // seqs
    )

    def factor_slice(ref, layer, g, start, size):
        at = pl.multiple_of(g * factor_rows, factor_rows)
        return ref[layer, pl.ds(at, factor_rows), pl.ds(start, size)]

    def low_start(layer, g, features):
        local_low = lax.dot_general(
            factor_slice(fin_ref, layer, g, 0, width),
            features,
            (((1,), (1,)), ((), ())),
            preferred_element_type=f32,
        )
        local_low = jnp.where(mask, local_low, 0.0)
        packed = local_low[:8]
        for at in range(8, factor_rows, 8):
            packed = packed + local_low[at : at + 8]
        small_start(layer, g, packed)

    def low_ready(layer, g):
        packed = small_sum(layer, g)
        low = jnp.concatenate([packed] * (factor_rows // 8), axis=0)
        low = jnp.where(mask, low, 0.0) * coef
        top = low.astype(bf16).astype(f32)
        blank = jnp.zeros((lanes - 2 * factor_rows, rows), f32)
        lows[g] = jnp.concatenate([top, low - top, blank], axis=0).T.astype(bf16)

    def correction(layer, g, p):
        start = pl.multiple_of(me * width + p * piece, lanes)
        factor = factor_slice(fout_ref, layer, g, start, piece)
        right = jnp.concatenate(
            [factor, factor, jnp.zeros((lanes - 2 * factor_rows, piece), bf16)], axis=0
        )
        return jnp.dot(lows[g], right, preferred_element_type=f32)

    def recur(layer, g, p, inputs):
        decay = decay_ref[layer : layer + 1, halves[p]]
        kept = 1.0 - decay
        carried = jnp.zeros((group, piece), f32)
        for t in range(steps):
            at = slice(t * group, (t + 1) * group)
            carried = decay * carried + kept * inputs[at]
            states[g, at, halves[p]] = carried
            powers = carried * carried
            total = powers[:, :lanes]
            for c in range(lanes, piece, lanes):
                total = total + powers[:, c : c + lanes]
            if p:
                total = total + squares[g, at, :]
            squares[g, at, :] = total

    def squares_start(layer, g):
        total = squares[g].T
        packed = total[:8]
        for at in range(8, lanes, 8):
            packed = packed + total[at : at + 8]
        small_start(2 + layer, g, packed)

    def normed(layer, g):
        squares = jnp.sum(small_sum(2 + layer, g), axis=0, keepdims=True)
        scale = lax.rsqrt(squares / full + norm_eps)
        scale = jnp.broadcast_to(scale, (lanes, rows)).T
        scale = jnp.concatenate([scale] * (width // lanes), axis=1)
        gain = gain_ref[layer : layer + 1, :]
        return (hidden[g].astype(f32) + states[g, :rows] * scale * gain).astype(bf16)

    def put_first(cols, value):
        states[0, :vocab, cols] = value

    exchange(
        0,
        lambda: embed_ref[...],
        vocab,
        0,
        lambda slot: weight_copy(0, slot).wait(),
        put_first,
    )
    for slot in range(4):
        weight_copy(1, slot).start()
    fout_load.wait()
    lax.fori_loop(0, chunks, unpack, 0)
    send_with(out_copy)

    def begin(g, carry):
        tokens = jnp.concatenate(
            [ids_ref[g * member_rows + m] for m in range(member_rows)], axis=0
        )
        entries = lax.broadcasted_iota(jnp.int32, (group, vocab), 1)
        for t in range(steps):
            onehot_ref[g, t * group : (t + 1) * group, :] = jnp.where(
                tokens[:, t : t + 1] == entries, 1.0, 0.0
            ).astype(bf16)
        features = jnp.dot(onehot_ref[g], embed_ref[...], preferred_element_type=f32).astype(bf16)
        hidden[g] = features
        low_start(0, g, features)
        return carry

    lax.fori_loop(0, chunks, begin, 0)
    shape_ranks()
    send_with(in_copy)
    for copy in self_copies():
        copy.start()
    for slot in range(4):
        weight_copy(1, slot).wait()

    def low_zero(g, carry):
        low_ready(0, g)
        return carry

    lax.fori_loop(0, chunks, low_zero, 0)
    for p in range(parts):
        whole = states[0, :vocab, halves[p]] + received(0, vocab, p)
        top = whole.astype(bf16)
        rest = (whole - top.astype(f32)).astype(bf16)

        def layer_zero(g, carry, p=p, top=top, rest=rest):
            picks = onehot_ref[g]
            inputs = (
                jnp.dot(picks, top, preferred_element_type=f32)
                + jnp.dot(picks, rest, preferred_element_type=f32)
                + correction(0, g, p)
            )
            recur(0, g, p, inputs)
            if p == parts - 1:
                squares_start(0, g)
            return carry

        for g in range(chunks):
            layer_zero(g, 0)

    def between(g, carry):
        hidden[g] = normed(0, g)

        def put(cols, value):
            states[g, :rows, cols] = value

        exchange(1 + g, lambda: hidden[g], rows, 1, lambda slot: None, put)
        low_start(1, g, hidden[g])
        return carry

    lax.fori_loop(0, chunks, between, 0)

    def layer_one(g, carry):
        low_ready(1, g)
        for p in range(parts):
            inputs = states[g, :rows, halves[p]] + received(1 + g, rows, p) + correction(1, g, p)
            recur(1, g, p, inputs)
        squares_start(1, g)
        return carry

    def finish(g, carry):
        last = normed(1, g)
        ending = last[rows - group :].astype(f32)
        for m in range(member_rows):
            final_ref[g * member_rows + m] = ending[m * seqs : (m + 1) * seqs].astype(bf16)
        total = last[:group].astype(f32)
        for t in range(1, steps):
            total = total + last[t * group : (t + 1) * group].astype(f32)
        total = total * reward_ref[...]
        packed = total[:, :lanes]
        for t in range(1, width // lanes):
            packed = packed + total[:, t * lanes : (t + 1) * lanes]
        marks[g, 0] = packed
        for r in range(3):
            mark_copy(g, r).start()
        return carry

    lax.fori_loop(0, chunks, lambda g, carry: finish(g, layer_one(g, carry)), 0)

    lane = lax.broadcasted_iota(jnp.int32, (seqs, lanes), 1)

    def collect(g, scores):
        for r in range(3):
            mark_copy(g, r).wait_recv()
        total = (marks[g, 0] + marks[g, 1]) + (marks[g, 2] + marks[g, 3])
        total = jnp.sum(total, axis=1, keepdims=True) * (full ** (-0.5) / steps)
        for m in range(member_rows):
            scores = jnp.where(
                lane == g * member_rows + m, total[m * seqs : (m + 1) * seqs], scores
            )
        for r in range(3):
            mark_copy(g, r).wait_send()
            for kind in range(4):
                small_copy(kind, g, r).wait_send()
        return scores

    score_ref[...] = lax.fori_loop(0, chunks, collect, jnp.zeros((seqs, lanes), f32))

    def drain(k, carry):
        for p in range(parts):
            pair_copy(k, 0, p).wait_send()
            pair_copy(k, 1, p).wait_send()
            cross_copy(k, p).wait_send()
        return carry

    lax.fori_loop(0, chunks + 1, drain, 0)

    def drain_pop(hop, carry):
        source = lax.rem(mine + pop - hop, pop)
        in_copy(hop, source).wait_recv()
        out_copy(hop, source).wait_recv()
        for make in (rank_copy, in_copy, out_copy):
            make(hop, mine).wait_send()
        return carry

    lax.fori_loop(1, pop, drain_pop, 0)
    for copy in self_copies():
        copy.wait()


def shards(
    token_ids,
    fitness_ranks,
    embedding,
    mix_weights,
    factors_in,
    factors_out,
    decay_rates,
    norm_gain,
    reward_dir,
):
    members, seqs, steps = token_ids.shape
    vocab, width = embedding.shape
    layers, _, full = mix_weights.shape
    rank = factors_in.shape[2]
    pop = lax.axis_size("pop")
    members_all = members * pop
    coef = noise_scale * (full * rank) ** (-0.5)
    columns = full // pop
    member_rows = 16 // seqs
    chunks = members // member_rows
    group = member_rows * seqs
    rows = group * steps
    local = members * rank
    dims = (pop, chunks, group, steps, member_rows, seqs, rank, width, full, coef)
    vmem = pl.BlockSpec(memory_space=pltpu.VMEM)
    smem = pl.BlockSpec(memory_space=pltpu.SMEM)
    hbm = pl.BlockSpec(memory_space=pl.ANY)
    most = max(rows, vocab)
    phases = chunks + 1
    parts = 4
    dma = pltpu.SemaphoreType.DMA
    final_features, marks, gin, gout = pl.pallas_call(
        functools.partial(policy_kernel, dims),
        out_shape=(
            jax.ShapeDtypeStruct((members, seqs, width), bf16),
            jax.ShapeDtypeStruct((seqs, lanes), f32),
            jax.ShapeDtypeStruct((layers, pop * local, width), bf16),
            jax.ShapeDtypeStruct((layers, pop * local, columns), bf16),
        ),
        in_specs=[vmem, vmem, hbm, vmem, hbm, smem, vmem, vmem, vmem],
        out_specs=(vmem, vmem, hbm, hbm),
        scratch_shapes=[
            pltpu.VMEM((layers, 4, width, width), bf16),
            pltpu.VMEM((phases, 2, parts, most, width // parts), bf16),
            pltpu.VMEM((phases, 2, parts, most, width // parts), bf16),
            pltpu.VMEM((phases, parts, most, width // parts), bf16),
            pltpu.VMEM((phases, parts, most, width // parts), bf16),
            pltpu.VMEM((chunks, most, width), f32),
            pltpu.VMEM((chunks, rows, width), bf16),
            pltpu.VMEM((chunks, rows, vocab), bf16),
            pltpu.VMEM((layers, members, rank, full), bf16),
            pltpu.VMEM((layers, local, width), bf16),
            pltpu.VMEM((layers, local, full), bf16),
            pltpu.VMEM((layers, local, width), bf16),
            pltpu.VMEM((8, lanes), jnp.int32),
            pltpu.VMEM((pop, 8, lanes), jnp.int32),
            pltpu.VMEM((chunks, rows, lanes), bf16),
            pltpu.VMEM((chunks, rows, lanes), f32),
            pltpu.VMEM((4, chunks, 4, 8, rows), f32),
            pltpu.VMEM((chunks, 4, group, lanes), f32),
            dma((layers, 4)),
            dma((phases, 2, parts)),
            dma((phases, 2, parts)),
            dma((phases, parts)),
            dma((phases, parts)),
            dma((4, chunks, 3)),
            dma((4, chunks, 3)),
            dma((chunks, 3)),
            dma((chunks, 3)),
            dma((3, pop)),
            dma((3, pop)),
            dma((2,)),
            dma,
        ],
        compiler_params=pltpu.CompilerParams(
            collective_id=0, has_side_effects=True, vmem_limit_bytes=60 * 1024 * 1024
        ),
    )(
        token_ids,
        embedding,
        mix_weights,
        factors_in,
        factors_out,
        fitness_ranks,
        decay_rates,
        norm_gain,
        reward_dir.reshape(1, width),
    )
    scores = marks[:, :members].T
    weight_delta = jnp.einsum("lki,lko->lio", gin, gout, preferred_element_type=f32)
    weight_step = weight_delta * (members_all * rank) ** (-0.5)
    return (final_features, scores, weight_step)


def solution(mesh):
    return jax.shard_map(
        shards,
        mesh=mesh,
        in_specs=(
            P("pop", None, None),
            P("pop"),
            P(None, "mp"),
            P(None, "mp", None),
            P(None, "pop", None, "mp"),
            P(None, "pop", None, None),
            P(None, "mp"),
            P(None, "mp"),
            P("mp"),
        ),
        out_specs=(P("pop", None, "mp"), P("pop", None), P(None, "mp", "pop")),
        check_vma=False,
    )
```
